512 devices in a mesh: dp: 32 (over y, x), seq: 16 (over z, core).
Axes of the slice: x: 4, y: 8, z: 8, core: 2. Of those that a mesh axis runs over, the one named last changes fastest.
Arguments:
- states: bfloat16 [65536, 1280], P(('dp', 'seq')), parts along dimension 0, may hold values from -90 to 90
- token_kind: int32 [65536], P(('dp', 'seq')), parts along dimension 0, may hold values from 0 to 3
- episode: int32 [65536], P(('dp', 'seq')), parts along dimension 0, may hold values from 0 to 3, never falling along the last dimension, each value on 1 to 1536 neighbouring positions
- kind_table: bfloat16 [4, 1280], replicated, may hold values from -3 to 3
- w_qkv: bfloat16 [1280, 3072], replicated, may hold values from -0.15625 to 0.15625
- w_out: bfloat16 [1024, 1280], replicated, may hold values from -0.1875 to 0.1875
Outputs:
- attended: bfloat16 [65536, 1280], P(('dp', 'seq')), parts along dimension 0
The draws below stay inside these ranges and needn't reach their ends.
There are 32 independent parts, one for each index of `dp`. The reference program is written for one: setup_inputs(seed, part) draws one part's arguments, and reference() takes and returns one part's arrays. A program takes and returns all parts, laid end to end along the dimension named above; an argument that names none is the same for every part. Nothing has to cross between parts.
All inputs are finite; a program needn't handle non-finite values.
Results may differ from the reference program's by a relative error of at most 0.0055.
The reference program's roundings to bfloat16 on the way (of `inputs`, `projected` and `heads_out`) count: a program that leaves them out, or rounds other values in their place, can miss the bound.
Values may be sent and summed in bfloat16 or wider, within the bound.
A program may use at most 128 MiB of HBM per device.

```python
import math
import jax
import jax.numpy as jnp
import numpy as np
from jax import lax

D = 1280
HEADS = 16
HD = 64
TYPES = 4
EPISODES = 4
SEQ = 2048


def draw_states(key, part):
    normal_part = jnp.clip(jax.random.normal(key, (SEQ, D), jnp.float32), -6.0, 6.0)
    return normal_part.astype(jnp.bfloat16)


def plant(result, key, smallest, top_value):
    dims = result.shape
    spot = [jax.random.randint(jax.random.fold_in(key, axis), (), 0, dims[axis]) for axis in range(len(dims))]
    result = result.at[tuple(spot)].set(smallest)
    longest = dims.index(max(dims))
    spot[longest] = (spot[longest] + 1) % dims[longest]
    return result.at[tuple(spot)].set(top_value)


def split_up(count, total, limit, slope):
    weights = [(1 << 20) // math.isqrt(grade ** slope) + 1 for grade in range(2, count + 1)]
    surplus, counts = total - limit - (count - 1), [1] * (count - 1)
    while surplus > 0:
        movable = [i for i in range(count - 1) if counts[i] < limit]
        mass, budget = sum([weights[i] for i in movable]), surplus
        for i in movable:
            extra = min(limit - counts[i], max(1, budget * weights[i] // mass), surplus)
            counts[i] = counts[i] + extra
            surplus = surplus - extra
    return np.array([limit] + counts)


def uneven_parts(key, number_of, total, reach, slope):
    if number_of == 2:
        one = jax.random.randint(key, (), max(1, total - reach), min(reach, total - 1) + 1)
        return jnp.stack([one, total - one])
    sizes = jnp.asarray(split_up(number_of, total, reach, slope), jnp.int32)
    twos = (number_of - 1) // 2
    donor, receiver = sizes[1:1 + 2 * twos:2], sizes[2:2 + 2 * twos:2]
    slack = jnp.minimum(donor - 1, reach - receiver)
    moved = jax.random.randint(jax.random.fold_in(key, 1), (twos,), 0, 1 << 20) % (slack + 1)
    sizes = sizes.at[1:1 + 2 * twos:2].set(donor - moved).at[2:2 + 2 * twos:2].set(receiver + moved)
    return sizes[jax.random.permutation(jax.random.fold_in(key, 2), number_of)]


def noise(rng, shape, scale, most, kind=jnp.bfloat16):
    values = jax.random.normal(rng, shape, jnp.float32) * scale
    return jnp.minimum(jnp.maximum(values, -most), most).astype(kind)


def setup_inputs(seed: int = 0, part: int = 0) -> dict:
    seeds = jax.random.split(jax.random.key(seed), 7)
    part_keys = jax.random.split(jax.random.fold_in(seeds[6], part), 7)
    states = draw_states(jax.random.fold_in(jax.random.fold_in(seeds[6], part), 71), part)
    token_kind = plant(jax.random.randint(part_keys[1], (SEQ,), 0, TYPES), jax.random.fold_in(part_keys[1], 1), 0, TYPES - 1).astype(jnp.int32)
    episode = jnp.searchsorted(jnp.cumsum(uneven_parts(part_keys[2], EPISODES, SEQ, SEQ * 3 // 4, 0)), jnp.arange(SEQ), side="right").astype(jnp.int32)
    kind_table = noise(seeds[3], (TYPES, D), 0.5, 3.0)
    w_qkv = noise(seeds[4], (D, 3 * HEADS * HD), D ** -0.5, 0.15625)
    w_out = noise(seeds[5], (HEADS * HD, D), (HEADS * HD) ** -0.5, 0.1875)
    return dict(states=states, token_kind=token_kind, episode=episode, kind_table=kind_table, w_qkv=w_qkv, w_out=w_out)


def reference(states, token_kind, episode, kind_table, w_qkv, w_out):
    inputs = (states.astype(jnp.float32) + kind_table.astype(jnp.float32)[token_kind]).astype(jnp.bfloat16)
    projected = jnp.dot(inputs, w_qkv, preferred_element_type=jnp.float32).astype(jnp.bfloat16)
    inner = HEADS * HD
    queries = projected[:, :inner].reshape(SEQ, HEADS, HD).astype(jnp.float32)
    key_rows = projected[:, inner:2 * inner].reshape(SEQ, HEADS, HD).astype(jnp.float32)
    value_rows = projected[:, 2 * inner:].reshape(SEQ, HEADS, HD).astype(jnp.float32)
    places = jnp.arange(SEQ, dtype=jnp.int32)
    stride = math.gcd(SEQ, 512)
    temper = 1.0 / math.sqrt(HD)

    def block(offset):
        block_q = lax.dynamic_slice_in_dim(queries, offset, stride, 0)
        block_place = lax.dynamic_slice_in_dim(places, offset, stride, 0)
        block_episode = lax.dynamic_slice_in_dim(episode, offset, stride, 0)
        scores = jnp.einsum('qhd,khd->hqk', block_q, key_rows) * temper
        allowed = (places[None, :] <= block_place[:, None]) & (episode[None, :] == block_episode[:, None])
        scores = jnp.where(allowed[None], scores, -1e+30)
        highest = lax.optimization_barrier(jnp.max(scores, axis=2))
        weights = jnp.where(allowed[None], jnp.exp(scores - highest[:, :, None]), 0.0)
        totals = lax.optimization_barrier(jnp.sum(weights, axis=2))
        summed = jnp.einsum('hqk,khd->qhd', weights.astype(jnp.bfloat16).astype(jnp.float32), value_rows)
        return (summed / totals.T[:, :, None]).astype(jnp.bfloat16).reshape(stride, inner)
    offsets = (jnp.arange(SEQ // stride, dtype=jnp.int32) * stride).astype(jnp.int32)
    heads_out = lax.map(block, offsets).reshape(SEQ, inner)
    return jnp.dot(heads_out, w_out, preferred_element_type=jnp.float32).astype(jnp.bfloat16)
```

```python
import functools

import jax
import jax.numpy as jnp
from jax import lax
from jax.experimental import pallas as pl
from jax.experimental.pallas import tpu as pltpu
from jax.sharding import PartitionSpec as P

HEADS = 16
MESH = pl.DeviceIdType.MESH
BF16 = jnp.bfloat16
F32 = jnp.float32
FAR = -1e30


def turn(k):
    return jnp.where(k % 2 == 1, (7 - k) // 2, 4 + k // 2)


def kernel(
    states_ref, kind_ref, episode_ref, table_ref, w_qkv_ref, w_out_ref, out_ref,
    x_ref, w_ref, wo_ref, kv_stage, q_stage, o_stage, kv_buf, q_buf, ep_buf, o_buf, k_aug, q_aug, s_ref,
    w_sem, wo_sem, kv_send, kv_recv, q_send, q_recv, ep_send, ep_recv, o_send, o_recv,
):
    rows, width = states_ref.shape
    inner = w_out_ref.shape[0]
    size = inner // HEADS
    pair = 2 * size
    me = lax.axis_index("seq")
    z, c = me // 2, me % 2

    barrier = pltpu.get_barrier_semaphore()

    def greet(k, _):
        pl.semaphore_signal(barrier, inc=1, device_id={"seq": (me + k) % HEADS}, device_id_type=MESH)
        return 0

    lax.fori_loop(1, HEADS, greet, 0)

    def chip(k):
        return (z + turn(k)) % 8

    def weights(k, part):
        at = pl.multiple_of(part * inner + chip(k) * pair, pair)
        return pltpu.make_async_copy(w_qkv_ref.at[:, pl.ds(at, pair)], w_ref.at[part, k], w_sem.at[part, k])

    def fetch_kv(k, _):
        weights(k, 1).start()
        weights(k, 2).start()
        return 0

    def fetch_q(k, _):
        weights(k, 0).start()
        return 0

    lax.fori_loop(0, 8, fetch_kv, 0)
    lax.fori_loop(0, 8, fetch_q, 0)
    w_out_copy = pltpu.make_async_copy(w_out_ref, wo_ref, wo_sem)
    w_out_copy.start()

    kinds = jnp.broadcast_to(kind_ref[...].astype(F32), (rows, rows)).T
    for at in range(0, width, rows):
        table = table_ref[:, at : at + rows].astype(F32)
        added = jnp.broadcast_to(table[3:4], (rows, rows))
        for kind in range(3):
            added = jnp.where(kinds == float(kind), table[kind : kind + 1], added)
        x_ref[:, at : at + rows] = (states_ref[:, at : at + rows].astype(F32) + added).astype(BF16)

    pl.semaphore_wait(barrier, HEADS - 1)

    ep_buf[me] = episode_ref[...]

    def episode_copy(k):
        return pltpu.make_async_remote_copy(
            src_ref=episode_ref, dst_ref=ep_buf.at[me], send_sem=ep_send.at[k], recv_sem=ep_recv.at[me],
            device_id={"seq": (me + k) % HEADS}, device_id_type=MESH,
        )

    def send_episode(k, _):
        episode_copy(k).start()
        return 0

    lax.fori_loop(1, HEADS, send_episode, 0)

    def kv_copy(k, core):
        return pltpu.make_async_remote_copy(
            src_ref=kv_stage.at[k, core], dst_ref=kv_buf.at[me], send_sem=kv_send.at[k, core], recv_sem=kv_recv.at[me],
            device_id={"seq": chip(k) * 2 + core}, device_id_type=MESH,
        )

    def q_copy(k, core):
        return pltpu.make_async_remote_copy(
            src_ref=q_stage.at[k, core], dst_ref=q_buf.at[me], send_sem=q_send.at[k, core], recv_sem=q_recv.at[me],
            device_id={"seq": chip(k) * 2 + core}, device_id_type=MESH,
        )

    def project(k, part):
        weights(k, part).wait()
        return jnp.dot(x_ref[...], w_ref[part, k], preferred_element_type=F32).astype(BF16).T

    def make_kv(k):
        keys = project(k, 1)
        values = project(k, 2)
        for core in range(2):
            kv_stage[k, core, :size] = keys[core * size : (core + 1) * size]
            kv_stage[k, core, size:] = values[core * size : (core + 1) * size]

    def make_q(k):
        queries = project(k, 0)
        for core in range(2):
            q_stage[k, core] = queries[core * size : (core + 1) * size]

    def do_kv(k, _):
        make_kv(k)
        kv_copy(k, 0).start()
        kv_copy(k, 1).start()
        return 0

    def do_q(k, _):
        make_q(k)
        q_copy(k, 0).start()
        q_copy(k, 1).start()
        return 0

    lax.fori_loop(0, 7, do_kv, 0)
    make_kv(7)
    kv_copy(7, 1 - c).start()
    kv_buf[me] = kv_stage[7, c]
    lax.fori_loop(0, 7, do_q, 0)
    make_q(7)
    q_copy(7, 1 - c).start()
    q_buf[me] = q_stage[7, c]

    def arrived(copy, j):
        @pl.when(j != me)
        def _():
            copy.wait_recv()

    def from_peer(dst, sem, j):
        return pltpu.make_async_remote_copy(
            src_ref=dst.at[j], dst_ref=dst.at[j], send_sem=sem.at[j], recv_sem=sem.at[j],
            device_id={"seq": j}, device_id_type=MESH,
        )

    lines = lax.broadcasted_iota(jnp.int32, (size, rows), 0)

    def take_kv(j, _):
        arrived(from_peer(ep_buf, ep_recv, j), j)
        arrived(from_peer(kv_buf, kv_recv, j), j)
        other = jnp.where((lines < 4) & (lines != ep_buf[j]), 1.0, 0.0).astype(BF16)
        k_aug[pl.ds(pl.multiple_of(j * rows, rows), rows)] = jnp.concatenate([kv_buf[j, :size], other], axis=0).T
        return 0

    def take_q(j, _):
        arrived(from_peer(q_buf, q_recv, j), j)
        same = jnp.where(lines == ep_buf[j], FAR, 0.0).astype(BF16)
        q_aug[j] = jnp.concatenate([q_buf[j] * 0.125, same], axis=0)
        return 0

    lax.fori_loop(0, HEADS, take_kv, 0)
    lax.fori_loop(0, HEADS, take_q, 0)

    block = 2 * rows
    later = lax.broadcasted_iota(jnp.int32, (block, block), 0) > lax.broadcasted_iota(jnp.int32, (block, block), 1)

    def o_copy(b, core):
        return pltpu.make_async_remote_copy(
            src_ref=o_stage.at[b, core], dst_ref=o_buf.at[me], send_sem=o_send.at[b, core], recv_sem=o_recv.at[me],
            device_id={"seq": 2 * b + core}, device_id_type=MESH,
        )

    for b in range(8):
        queries = jnp.concatenate([q_aug[2 * b], q_aug[2 * b + 1]], axis=1)
        top = None
        for a in range(b + 1):
            scores = jnp.dot(k_aug[a * block : (a + 1) * block], queries, preferred_element_type=F32)
            if a == b:
                scores = jnp.where(later, FAR, scores)
            s_ref[a * block : (a + 1) * block] = scores
            here = jnp.max(scores.reshape(block // 8, 8, block), axis=0)
            top = here if top is None else jnp.maximum(top, here)
        top = jnp.max(top, axis=0, keepdims=True)
        total, summed = None, None
        for a in range(b + 1):
            weight = jnp.exp(s_ref[a * block : (a + 1) * block] - top)
            part = jnp.sum(weight.reshape(block // 8, 8, block), axis=0)
            values = jnp.concatenate([kv_buf[2 * a, size:], kv_buf[2 * a + 1, size:]], axis=1)
            mixed = jnp.dot(values, weight.astype(BF16), preferred_element_type=F32)
            total = part if total is None else total + part
            summed = mixed if summed is None else summed + mixed
        total = jnp.sum(total, axis=0, keepdims=True)
        result = (summed / total).astype(BF16)
        for core in range(2):
            o_stage[b, core] = result[:, core * rows : (core + 1) * rows]

            @pl.when(2 * b + core != me)
            def _():
                o_copy(b, core).start()

            @pl.when(2 * b + core == me)
            def _():
                o_buf[me] = o_stage[b, core]

    def take_o(j, _):
        arrived(from_peer(o_buf, o_recv, j), j)
        return 0

    lax.fori_loop(0, HEADS, take_o, 0)
    w_out_copy.wait()
    heads_out = o_buf[...].reshape(inner, rows).T
    out_ref[...] = jnp.dot(heads_out, wo_ref[...], preferred_element_type=F32).astype(BF16)

    def sent(k, _):
        kv_copy(k, 0).wait_send()
        kv_copy(k, 1).wait_send()
        q_copy(k, 0).wait_send()
        q_copy(k, 1).wait_send()
        return 0

    def episode_sent(k, _):
        episode_copy(k).wait_send()
        return 0

    def o_sent(b, _):
        for core in range(2):
            @pl.when(2 * b + core != me)
            def _():
                o_copy(b, core).wait_send()
        return 0

    lax.fori_loop(1, HEADS, episode_sent, 0)
    lax.fori_loop(0, 7, sent, 0)
    kv_copy(7, 1 - c).wait_send()
    q_copy(7, 1 - c).wait_send()
    lax.fori_loop(0, 8, o_sent, 0)


def local(states, token_kind, episode, kind_table, w_qkv, w_out):
    rows, width = states.shape
    inner = w_out.shape[0]
    size = inner // HEADS
    vmem = pl.BlockSpec(memory_space=pltpu.VMEM)
    hbm = pl.BlockSpec(memory_space=pl.ANY)
    dma = pltpu.SemaphoreType.DMA
    return pl.pallas_call(
        kernel,
        name="episode_attention",
        out_shape=jax.ShapeDtypeStruct((rows, width), BF16),
        in_specs=[vmem, vmem, vmem, vmem, hbm, hbm],
        out_specs=vmem,
        scratch_shapes=[
            pltpu.VMEM((rows, width), BF16),
            pltpu.VMEM((3, 8, width, 2 * size), BF16),
            pltpu.VMEM((inner, width), BF16),
            pltpu.VMEM((8, 2, 2 * size, rows), BF16),
            pltpu.VMEM((8, 2, size, rows), BF16),
            pltpu.VMEM((8, 2, size, rows), BF16),
            pltpu.VMEM((HEADS, 2 * size, rows), BF16),
            pltpu.VMEM((HEADS, size, rows), BF16),
            pltpu.VMEM((HEADS, 1, rows), jnp.int32),
            pltpu.VMEM((HEADS, size, rows), BF16),
            pltpu.VMEM((HEADS * rows, 2 * size), BF16),
            pltpu.VMEM((HEADS, 2 * size, rows), BF16),
            pltpu.VMEM((HEADS * rows, 2 * rows), F32),
            dma((3, 8)), dma(()),
            dma((8, 2)), dma((HEADS,)),
            dma((8, 2)), dma((HEADS,)),
            dma((HEADS,)), dma((HEADS,)),
            dma((8, 2)), dma((HEADS,)),
        ],
        compiler_params=pltpu.CompilerParams(
            collective_id=0, has_side_effects=True, vmem_limit_bytes=48 * 1024 * 1024
        ),
    )(states, token_kind.reshape(1, rows), episode.reshape(1, rows), kind_table, w_qkv, w_out)


def solution(mesh):
    placed = (P(("dp", "seq"), None), P(("dp", "seq")), P(("dp", "seq")), P(), P(), P())
    return jax.shard_map(
        local, mesh=mesh, in_specs=placed, out_specs=P(("dp", "seq"), None), check_vma=False
    )
```

```python
import jax
import jax.numpy as jnp
from jax import lax
from jax.experimental import pallas as pl
from jax.experimental.pallas import tpu as pltpu
from jax.sharding import PartitionSpec as P

HEADS = 16
CHIPS = 8
MESH = pl.DeviceIdType.MESH
BF16 = jnp.bfloat16
F32 = jnp.float32
FAR = -1e30
AHEAD = 4


def turn(k):
    return jnp.where(k % 2 == 1, (7 - k) // 2, 4 + k // 2)


def kernel(
    states_hbm, kind_hbm, episode_hbm, table_hbm, w_qkv_hbm, w_out_hbm, out_ref,
    states_ref, kind_ref, table_ref, x_ref, w_ref, wo_ref, kv_stage, q_stage, o_stage, kv_buf, q_buf, ep_buf, o_buf,
    k_aug, s_ref, p_ref, v_ref, h_ref, acc_ref,
    in_sem, w_sem, kv_send, kv_recv, q_send, q_recv, ep_send, ep_recv, o_send, o_recv,
):
    rows, width = states_ref.shape
    inner = wo_ref.shape[0]
    size = inner // HEADS
    pair = 2 * size
    block = 2 * rows
    me = lax.axis_index("seq")
    z, c = me // 2, me % 2

    barrier = pltpu.get_barrier_semaphore()

    def greet(k, _):
        pl.semaphore_signal(barrier, inc=1, device_id={"seq": (me + k) % HEADS}, device_id_type=MESH)
        return 0

    lax.fori_loop(1, HEADS, greet, 0)

    loads = [
        pltpu.make_async_copy(states_hbm, states_ref, in_sem.at[0]),
        pltpu.make_async_copy(kind_hbm, kind_ref, in_sem.at[1]),
        pltpu.make_async_copy(table_hbm, table_ref, in_sem.at[2]),
        pltpu.make_async_copy(episode_hbm, ep_buf.at[me], in_sem.at[3]),
    ]

    def w_out_copy(slot):
        g = to_chip((slot + 7) % CHIPS)
        return pltpu.make_async_copy(
            w_out_hbm.at[pl.ds(pl.multiple_of(g * pair, pair), pair)],
            wo_ref.at[pl.ds(pl.multiple_of(slot * pair, pair), pair)], in_sem.at[4],
        )

    for load in loads:
        load.start()

    def to_chip(k):
        return (z + turn(k)) % CHIPS

    def from_chip(k):
        return (z + CHIPS - turn(k)) % CHIPS

    def weights(k, part):
        at = pl.multiple_of(part * inner + to_chip(k) * pair, pair)
        return pltpu.make_async_copy(
            w_qkv_hbm.at[:, pl.ds(at, pair)], w_ref.at[part, k], w_sem.at[0 if part == 0 else 1, k]
        )

    def landed(ref, sem):
        pltpu.make_async_copy(ref, ref, sem).wait()

    def fetch_kv(k, _):
        weights(k, 1).start()
        weights(k, 2).start()
        return 0

    lax.fori_loop(0, AHEAD, fetch_kv, 0)

    for load in loads:
        load.wait()
    kinds = jnp.broadcast_to(kind_ref[...].astype(F32), (rows, rows)).T
    for at in range(0, width, rows):
        table = table_ref[:, at : at + rows].astype(F32)
        added = jnp.broadcast_to(table[3:4], (rows, rows))
        for kind in range(3):
            added = jnp.where(kinds == float(kind), table[kind : kind + 1], added)
        x_ref[:, at : at + rows] = (states_ref[:, at : at + rows].astype(F32) + added).astype(BF16)

    def episode_copy(k):
        return pltpu.make_async_remote_copy(
            src_ref=ep_buf.at[me], dst_ref=ep_buf.at[me], send_sem=ep_send, recv_sem=ep_recv,
            device_id={"seq": (me + k) % HEADS}, device_id_type=MESH,
        )

    def kv_copy(k, core, lane=0):
        return pltpu.make_async_remote_copy(
            src_ref=kv_stage.at[k, core], dst_ref=kv_buf.at[me], send_sem=kv_send.at[lane], recv_sem=kv_recv.at[z],
            device_id={"seq": to_chip(k) * 2 + core}, device_id_type=MESH,
        )

    def q_copy(k, core, lane=0):
        return pltpu.make_async_remote_copy(
            src_ref=q_stage.at[k, core], dst_ref=q_buf.at[me], send_sem=q_send.at[lane], recv_sem=q_recv.at[z],
            device_id={"seq": to_chip(k) * 2 + core}, device_id_type=MESH,
        )

    def o_copy(b, core, lane=0):
        return pltpu.make_async_remote_copy(
            src_ref=o_stage.at[b, core], dst_ref=o_buf.at[me], send_sem=o_send.at[lane], recv_sem=o_recv.at[z],
            device_id={"seq": 2 * b + core}, device_id_type=MESH,
        )

    def project(k, part):
        return jnp.dot(x_ref[...], w_ref[part, k], preferred_element_type=F32).astype(BF16).T

    def make_kv(k):
        landed(w_ref.at[pl.ds(1, 2), k], w_sem.at[1, k])
        keys = project(k, 1)
        values = project(k, 2)
        for core in range(2):
            kv_stage[k, core, :size] = keys[core * size : (core + 1) * size]
            kv_stage[k, core, size:] = values[core * size : (core + 1) * size]

    def make_q(k):
        landed(w_ref.at[0, k], w_sem.at[0, k])
        queries = project(k, 0)
        for core in range(2):
            q_stage[k, core] = queries[core * size : (core + 1) * size]

    def fetch_later(k):
        @pl.when(k < CHIPS)
        def _():
            weights(k, 1).start()
            weights(k, 2).start()

        @pl.when((k >= CHIPS) & (k < 2 * CHIPS))
        def _():
            weights(k - CHIPS, 0).start()

    def send_kv(k, _):
        kv_copy(k, 0).start()
        kv_copy(k, 1).start()
        return 0

    def send_q(k, _):
        q_copy(k, 0).start()
        q_copy(k, 1).start()
        return 0

    def stage_kv(k, _):
        fetch_later(k + AHEAD)
        make_kv(k)
        return 0

    def stage_q(k, _):
        fetch_later(k + CHIPS + AHEAD)
        make_q(k)
        return 0

    def do_kv(k, _):
        stage_kv(k, 0)
        return send_kv(k, 0)

    def do_q(k, _):
        stage_q(k, 0)
        return send_q(k, 0)

    def send_episode(k, _):
        episode_copy(k).start()
        return 0

    kv_early = jnp.where(z < 4, 7, jnp.where(z < 7, 3, 1))
    q_early = jnp.where(z < 2, 7, jnp.where(z == 2, 3, 0))
    lax.fori_loop(0, kv_early, stage_kv, 0)

    @pl.when(z < 4)
    def _():
        stage_kv(7, 0)

    lax.fori_loop(0, q_early, stage_q, 0)

    pl.semaphore_wait(barrier, HEADS - 1)
    lax.fori_loop(1, HEADS, send_episode, 0)
    lax.fori_loop(0, kv_early, send_kv, 0)
    lax.fori_loop(kv_early, 7, do_kv, 0)

    @pl.when(z >= 4)
    def _():
        stage_kv(7, 0)

    kv_copy(7, 1 - c, 1).start()
    kv_buf[me] = kv_stage[7, c]
    lax.fori_loop(0, q_early, send_q, 0)
    lax.fori_loop(q_early, 7, do_q, 0)

    stage_q(7, 0)
    q_copy(7, 1 - c, 1).start()
    q_buf[me] = q_stage[7, c]

    def fetch_w_out(slot, _):
        w_out_copy(slot).start()
        return 0

    lax.fori_loop(0, CHIPS, fetch_w_out, 0)

    lines = lax.broadcasted_iota(jnp.int32, (size, rows), 0)

    def take_kv(j):
        other = jnp.where((lines < 4) & (lines != ep_buf[j]), 1.0, 0.0).astype(BF16)
        at = pl.multiple_of(j * rows, rows)
        k_aug[pl.ds(at, rows)] = jnp.concatenate([kv_buf[j, :size], other], axis=0).T
        v_ref[:, pl.ds(at, rows)] = kv_buf[j, size:]

    def take_chip(k, _):
        g = from_chip(k)
        landed(kv_buf.at[pl.ds(2 * g, 2)], kv_recv.at[g])
        take_kv(2 * g)
        take_kv(2 * g + 1)
        return 0

    partner = z * 2 + 1 - c
    landed(ep_buf.at[pl.ds(0, HEADS - 1)], ep_recv)
    take_kv(me)
    landed(kv_buf.at[partner], kv_recv.at[z])
    take_kv(partner)
    lax.fori_loop(0, 7, take_chip, 0)

    later = lax.broadcasted_iota(jnp.int32, (block, block), 0) > lax.broadcasted_iota(jnp.int32, (block, block), 1)

    def attend(b):
        queries = []
        for j in (2 * b, 2 * b + 1):
            same = jnp.where(lines == ep_buf[j], FAR, 0.0).astype(BF16)
            queries.append(jnp.concatenate([q_buf[j] * 0.125, same], axis=0))
        queries = jnp.concatenate(queries, axis=1)
        top = None
        for a in range(b + 1):
            scores = jnp.dot(k_aug[a * block : (a + 1) * block], queries, preferred_element_type=F32)
            if a == b:
                scores = jnp.where(later, FAR, scores)
            s_ref[a * block : (a + 1) * block] = scores
            here = jnp.max(scores.reshape(block // 8, 8, block), axis=0)
            top = here if top is None else jnp.maximum(top, here)
        top = jnp.max(top, axis=0, keepdims=True)
        total = None
        for a in range(b + 1):
            weight = jnp.exp(s_ref[a * block : (a + 1) * block] - top)
            here = jnp.sum(weight.reshape(block // 8, 8, block), axis=0)
            total = here if total is None else total + here
            p_ref[a * block : (a + 1) * block] = weight.astype(BF16)
        end = (b + 1) * block
        summed = jnp.dot(v_ref[:, :end], p_ref[:end], preferred_element_type=F32)
        total = jnp.sum(total, axis=0, keepdims=True)
        result = (summed / total).astype(BF16)
        for core in range(2):
            o_stage[b, core] = result[:, core * rows : (core + 1) * rows]

    def attend_any(b):
        lax.switch(b, [lambda b=b: attend(b) for b in range(CHIPS)])

    landed(q_buf.at[partner], q_recv.at[z])
    attend_any(z)
    o_copy(z, 1 - c, 1).start()
    o_buf[me] = o_stage[z, c]

    def answer(k, _):
        b = from_chip(k)
        landed(q_buf.at[pl.ds(2 * b, 2)], q_recv.at[b])
        attend_any(b)
        o_copy(b, 0).start()
        o_copy(b, 1).start()
        return 0

    lax.fori_loop(0, 7, answer, 0)

    def take_o(g, slot):
        h_ref[:, pl.ds(pl.multiple_of(slot * pair, pair), pair)] = jnp.concatenate(
            [o_buf[2 * g], o_buf[2 * g + 1]], axis=0
        ).T

    def take_chip_o(k, _):
        g = to_chip(k)
        landed(o_buf.at[pl.ds(2 * g, 2)], o_recv.at[g])
        take_o(g, k + 1)
        return 0

    landed(wo_ref, in_sem.at[4])
    landed(o_buf.at[partner], o_recv.at[z])
    take_o(z, 0)
    lax.fori_loop(0, 5, take_chip_o, 0)
    most = 6 * pair
    acc_ref[...] = jnp.dot(h_ref[:, :most], wo_ref[:most], preferred_element_type=F32)
    lax.fori_loop(5, 7, take_chip_o, 0)
    rest = jnp.dot(h_ref[:, most:], wo_ref[most:], preferred_element_type=F32)
    out_ref[...] = (acc_ref[...] + rest).astype(BF16)

    landed(ep_buf.at[pl.ds(0, HEADS - 1)], ep_send)
    landed(kv_stage.at[pl.ds(0, 7)], kv_send.at[0])
    landed(q_stage.at[pl.ds(0, 7)], q_send.at[0])
    landed(o_stage.at[pl.ds(0, 7)], o_send.at[0])
    landed(kv_stage.at[7, 0], kv_send.at[1])
    landed(q_stage.at[7, 0], q_send.at[1])
    landed(o_stage.at[7, 0], o_send.at[1])


def local(states, token_kind, episode, kind_table, w_qkv, w_out):
    rows, width = states.shape
    inner = w_out.shape[0]
    size = inner // HEADS
    hbm = pl.BlockSpec(memory_space=pltpu.HBM)
    dma = pltpu.SemaphoreType.DMA
    return pl.pallas_call(
        kernel,
        name="episode_attention",
        out_shape=jax.ShapeDtypeStruct((rows, width), BF16),
        in_specs=[hbm] * 6,
        out_specs=pl.BlockSpec(memory_space=pltpu.VMEM),
        scratch_shapes=[
            pltpu.VMEM((rows, width), BF16),
            pltpu.VMEM((1, rows), jnp.int32),
            pltpu.VMEM(kind_table.shape, BF16),
            pltpu.VMEM((rows, width), BF16),
            pltpu.VMEM((3, CHIPS, width, 2 * size), BF16),
            pltpu.VMEM((inner, width), BF16),
            pltpu.VMEM((CHIPS, 2, 2 * size, rows), BF16),
            pltpu.VMEM((CHIPS, 2, size, rows), BF16),
            pltpu.VMEM((CHIPS, 2, size, rows), BF16),
            pltpu.VMEM((HEADS, 2 * size, rows), BF16),
            pltpu.VMEM((HEADS, size, rows), BF16),
            pltpu.VMEM((HEADS, 1, rows), jnp.int32),
            pltpu.VMEM((HEADS, size, rows), BF16),
            pltpu.VMEM((HEADS * rows, 2 * size), BF16),
            pltpu.VMEM((HEADS * rows, 2 * rows), F32),
            pltpu.VMEM((HEADS * rows, 2 * rows), BF16),
            pltpu.VMEM((size, HEADS * rows), BF16),
            pltpu.VMEM((rows, inner), BF16),
            pltpu.VMEM((rows, width), F32),
            dma((5,)), dma((2, CHIPS)),
            dma((2,)), dma((CHIPS,)),
            dma((2,)), dma((CHIPS,)),
            dma(()), dma(()),
            dma((2,)), dma((CHIPS,)),
        ],
        compiler_params=pltpu.CompilerParams(
            collective_id=0, has_side_effects=True, vmem_limit_bytes=48000000
        ),
    )(*[pltpu.with_memory_space_constraint(v, pltpu.HBM) for v in (states, token_kind.reshape(1, rows), episode.reshape(1, rows), kind_table, w_qkv, w_out)])


def solution(mesh):
    placed = (P(("dp", "seq"), None), P(("dp", "seq")), P(("dp", "seq")), P(), P(), P())
    return jax.shard_map(
        local, mesh=mesh, in_specs=placed, out_specs=P(("dp", "seq"), None), check_vma=False
    )
```

```python
import jax
import jax.numpy as jnp
from jax import lax
from jax.experimental import pallas as pl
from jax.experimental.pallas import tpu as pltpu
from jax.sharding import PartitionSpec as P

HEADS = 16
CHIPS = 8
MESH = pl.DeviceIdType.MESH
BF16 = jnp.bfloat16
F32 = jnp.float32
FAR = -1e30
AHEAD = 4


NEAR = 4
OWN = CHIPS - 1


def packed(turns):
    return sum(turn << (3 * at) for at, turn in enumerate(turns))


KV_TURNS = packed((2, 6, 1, 7, 4, 3, 5, 0))
Q_TURNS = packed((4, 3, 5, 2, 6, 1, 7, 0))


def kernel(
    states_hbm, kind_hbm, episode_hbm, table_hbm, w_qkv_hbm, w_out_hbm, out_ref,
    states_ref, kind_ref, table_ref, x_ref, w_ref, wo_ref, kv_stage, q_stage, o_stage, kv_buf, q_buf, ep_buf, o_buf,
    k_aug, s_ref, v_ref, h_ref, acc_ref,
    in_sem, w_sem, beyond, kv_send, kv_recv, q_send, q_recv, ep_send, ep_recv, o_send, o_recv,
):
    rows, width = states_ref.shape
    inner = wo_ref.shape[0]
    size = inner // HEADS
    pair = 2 * size
    block = 2 * rows
    me = lax.axis_index("seq")
    z, c = me // 2, me % 2

    barrier = pltpu.get_barrier_semaphore()

    def greet(k, _):
        pl.semaphore_signal(barrier, inc=1, device_id={"seq": (2 * z + k) % HEADS}, device_id_type=MESH)
        return 0

    partner = z * 2 + 1 - c
    lax.fori_loop(2, 6, greet, 0)
    lax.fori_loop(HEADS - 4, HEADS, greet, 0)
    pl.semaphore_signal(barrier, inc=1, device_id={"seq": partner}, device_id_type=MESH)

    def tell(side, chips):
        pl.semaphore_signal(
            beyond.at[side], inc=1, device_id={"seq": (z + chips) % CHIPS * 2 + c}, device_id_type=MESH
        )

    loads = [
        pltpu.make_async_copy(states_hbm, states_ref, in_sem.at[0]),
        pltpu.make_async_copy(kind_hbm, kind_ref, in_sem.at[1]),
        pltpu.make_async_copy(table_hbm, table_ref, in_sem.at[2]),
        pltpu.make_async_copy(episode_hbm, ep_buf.at[me], in_sem.at[3]),
    ]

    def w_out_copy(slot):
        g = to_chip(Q_TURNS, (slot + OWN) % CHIPS)
        return pltpu.make_async_copy(
            w_out_hbm.at[pl.ds(pl.multiple_of(g * pair, pair), pair)],
            wo_ref.at[pl.ds(pl.multiple_of(slot * pair, pair), pair)], in_sem.at[4],
        )

    for load in loads:
        load.start()

    def to_chip(turns, k):
        return (z + ((turns >> (3 * k)) & 7)) % CHIPS

    def from_chip(turns, k):
        return (z + CHIPS - ((turns >> (3 * k)) & 7)) % CHIPS

    def weights(k, part):
        g = to_chip(KV_TURNS if part else Q_TURNS, k)
        at = pl.multiple_of(part * inner + g * pair, pair)
        return pltpu.make_async_copy(
            w_qkv_hbm.at[:, pl.ds(at, pair)], w_ref.at[part, k], w_sem.at[0 if part == 0 else 1, k]
        )

    def landed(ref, sem):
        pltpu.make_async_copy(ref, ref, sem).wait()

    def fetch_kv(k, _):
        weights(k, 1).start()
        weights(k, 2).start()
        return 0

    lax.fori_loop(0, AHEAD, fetch_kv, 0)

    for load in loads:
        load.wait()
    kinds = jnp.broadcast_to(kind_ref[...].astype(F32), (rows, rows)).T
    for at in range(0, width, rows):
        table = table_ref[:, at : at + rows].astype(F32)
        added = jnp.broadcast_to(table[3:4], (rows, rows))
        for kind in range(3):
            added = jnp.where(kinds == float(kind), table[kind : kind + 1], added)
        x_ref[:, at : at + rows] = (states_ref[:, at : at + rows].astype(F32) + added).astype(BF16)

    def episode_copy(k, core):
        return pltpu.make_async_remote_copy(
            src_ref=ep_buf.at[me], dst_ref=ep_buf.at[me], send_sem=ep_send, recv_sem=ep_recv,
            device_id={"seq": to_chip(KV_TURNS, k) * 2 + core}, device_id_type=MESH,
        )

    def kv_copy(k, core, lane=0):
        return pltpu.make_async_remote_copy(
            src_ref=kv_stage.at[k, core], dst_ref=kv_buf.at[me], send_sem=kv_send.at[lane], recv_sem=kv_recv.at[z],
            device_id={"seq": to_chip(KV_TURNS, k) * 2 + core}, device_id_type=MESH,
        )

    def q_copy(k, core, lane=0):
        return pltpu.make_async_remote_copy(
            src_ref=q_stage.at[k, core], dst_ref=q_buf.at[me], send_sem=q_send.at[lane], recv_sem=q_recv.at[z],
            device_id={"seq": to_chip(Q_TURNS, k) * 2 + core}, device_id_type=MESH,
        )

    def o_copy(b, core, lane=0):
        return pltpu.make_async_remote_copy(
            src_ref=o_stage.at[b, core], dst_ref=o_buf.at[me], send_sem=o_send.at[lane], recv_sem=o_recv.at[z],
            device_id={"seq": 2 * b + core}, device_id_type=MESH,
        )

    def project(k, part):
        return jnp.dot(x_ref[...], w_ref[part, k], preferred_element_type=F32).astype(BF16).T

    def make_kv(k):
        landed(w_ref.at[pl.ds(1, 2), k], w_sem.at[1, k])
        keys = project(k, 1)
        values = project(k, 2)
        for core in range(2):
            kv_stage[k, core, :size] = keys[core * size : (core + 1) * size]
            kv_stage[k, core, size:] = values[core * size : (core + 1) * size]

    def make_q(k):
        landed(w_ref.at[0, k], w_sem.at[0, k])
        queries = project(k, 0)
        for core in range(2):
            q_stage[k, core] = queries[core * size : (core + 1) * size]

    def fetch_later(k):
        @pl.when(k < CHIPS)
        def _():
            weights(k, 1).start()
            weights(k, 2).start()

        @pl.when((k >= CHIPS) & (k < 2 * CHIPS))
        def _():
            weights(k - CHIPS, 0).start()

    def send_kv(k, _):
        @pl.when(k == NEAR)
        def _():
            pl.semaphore_wait(beyond.at[0], 1)
            pl.semaphore_wait(beyond.at[1], 1)

        episode_copy(k, 0).start()
        episode_copy(k, 1).start()
        kv_copy(k, 0).start()
        kv_copy(k, 1).start()
        return 0

    def send_q(k, _):
        q_copy(k, 0).start()
        q_copy(k, 1).start()
        return 0

    def stage_kv(k, _):
        fetch_later(k + AHEAD)
        make_kv(k)
        return 0

    def stage_q(k, _):
        fetch_later(k + CHIPS + AHEAD)
        make_q(k)
        return 0

    def do_kv(k, _):
        stage_kv(k, 0)
        return send_kv(k, 0)

    def do_q(k, _):
        stage_q(k, 0)
        return send_q(k, 0)

    late = (z == 0) & (c == 0) & (lax.axis_index("dp") == 0)
    kv_early = jnp.where(z < 3, 7, jnp.where(z == 3, 5, jnp.where(z < 6, 2, 1)))
    kv_early = jnp.where(late, 2, kv_early)
    q_early = jnp.where((z < 2) & jnp.logical_not(late), 7, 0)
    own_early = (z < 3) & jnp.logical_not(late)
    lax.fori_loop(0, kv_early, stage_kv, 0)

    @pl.when(own_early)
    def _():
        stage_kv(7, 0)

    lax.fori_loop(0, q_early, stage_q, 0)

    pl.semaphore_wait(barrier, 9)
    tell(0, 2)
    tell(1, 6)
    lax.fori_loop(0, kv_early, send_kv, 0)
    lax.fori_loop(kv_early, 7, do_kv, 0)

    @pl.when(jnp.logical_not(own_early))
    def _():
        stage_kv(7, 0)

    episode_copy(7, 1 - c).start()
    kv_copy(7, 1 - c, 1).start()
    kv_buf[me] = kv_stage[7, c]
    lax.fori_loop(0, q_early, send_q, 0)
    lax.fori_loop(q_early, 7, do_q, 0)

    stage_q(7, 0)
    q_copy(7, 1 - c, 1).start()
    q_buf[me] = q_stage[7, c]

    def fetch_w_out(slot, _):
        w_out_copy(slot).start()
        return 0

    lax.fori_loop(0, CHIPS, fetch_w_out, 0)

    lines = lax.broadcasted_iota(jnp.int32, (size, rows), 0)

    def take_kv(j):
        other = jnp.where((lines < 4) & (lines != ep_buf[j]), 1.0, 0.0).astype(BF16)
        at = pl.multiple_of(j * rows, rows)
        k_aug[pl.ds(at, rows)] = jnp.concatenate([kv_buf[j, :size], other], axis=0).T
        v_ref[:, pl.ds(at, rows)] = kv_buf[j, size:]

    def take_chip(k, _):
        g = from_chip(KV_TURNS, k)
        landed(kv_buf.at[pl.ds(2 * g, 2)], kv_recv.at[g])
        take_kv(2 * g)
        take_kv(2 * g + 1)
        return 0

    landed(ep_buf.at[pl.ds(0, HEADS - 1)], ep_recv)
    take_kv(me)
    landed(kv_buf.at[partner], kv_recv.at[z])
    take_kv(partner)
    lax.fori_loop(0, 7, take_chip, 0)

    later = lax.broadcasted_iota(jnp.int32, (block, block), 0) > lax.broadcasted_iota(jnp.int32, (block, block), 1)

    def attend(b):
        queries = []
        for j in (2 * b, 2 * b + 1):
            same = jnp.where(lines == ep_buf[j], FAR, 0.0).astype(BF16)
            queries.append(jnp.concatenate([q_buf[j] * 0.125, same], axis=0))
        queries = jnp.concatenate(queries, axis=1)
        top = None
        for a in range(b + 1):
            scores = jnp.dot(k_aug[a * block : (a + 1) * block], queries, preferred_element_type=F32)
            if a == b:
                scores = jnp.where(later, FAR, scores)
            s_ref[a * block : (a + 1) * block] = scores
            here = jnp.max(scores.reshape(block // 8, 8, block), axis=0)
            top = here if top is None else jnp.maximum(top, here)
        top = jnp.max(top, axis=0, keepdims=True)
        total, summed = None, None
        for a in range(b + 1):
            weight = jnp.exp(s_ref[a * block : (a + 1) * block] - top)
            here = jnp.sum(weight.reshape(block // 8, 8, block), axis=0)
            total = here if total is None else total + here
            mixed = jnp.dot(v_ref[:, a * block : (a + 1) * block], weight.astype(BF16), preferred_element_type=F32)
            summed = mixed if summed is None else summed + mixed
        total = jnp.sum(total, axis=0, keepdims=True)
        result = (summed / total).astype(BF16)
        for core in range(2):
            o_stage[b, core] = result[:, core * rows : (core + 1) * rows]

    def attend_any(b):
        lax.switch(b, [lambda b=b: attend(b) for b in range(CHIPS)])

    landed(q_buf.at[partner], q_recv.at[z])
    attend_any(z)
    o_copy(z, 1 - c, 1).start()
    o_buf[me] = o_stage[z, c]

    def answer(k, _):
        b = from_chip(Q_TURNS, k)
        landed(q_buf.at[pl.ds(2 * b, 2)], q_recv.at[b])
        attend_any(b)
        o_copy(b, 0).start()
        o_copy(b, 1).start()
        return 0

    lax.fori_loop(0, 7, answer, 0)

    def take_o(g, slot):
        h_ref[:, pl.ds(pl.multiple_of(slot * pair, pair), pair)] = jnp.concatenate(
            [o_buf[2 * g], o_buf[2 * g + 1]], axis=0
        ).T

    def take_chip_o(k, _):
        g = to_chip(Q_TURNS, k)
        landed(o_buf.at[pl.ds(2 * g, 2)], o_recv.at[g])
        take_o(g, k + 1)
        return 0

    landed(wo_ref, in_sem.at[4])
    landed(o_buf.at[partner], o_recv.at[z])
    take_o(z, 0)
    lax.fori_loop(0, 5, take_chip_o, 0)
    most = 6 * pair
    acc_ref[...] = jnp.dot(h_ref[:, :most], wo_ref[:most], preferred_element_type=F32)
    lax.fori_loop(5, 7, take_chip_o, 0)
    rest = jnp.dot(h_ref[:, most:], wo_ref[most:], preferred_element_type=F32)
    out_ref[...] = (acc_ref[...] + rest).astype(BF16)

    landed(ep_buf.at[pl.ds(0, HEADS - 1)], ep_send)
    landed(kv_stage.at[pl.ds(0, 7)], kv_send.at[0])
    landed(q_stage.at[pl.ds(0, 7)], q_send.at[0])
    landed(o_stage.at[pl.ds(0, 7)], o_send.at[0])
    landed(kv_stage.at[7, 0], kv_send.at[1])
    landed(q_stage.at[7, 0], q_send.at[1])
    landed(o_stage.at[7, 0], o_send.at[1])


def local(states, token_kind, episode, kind_table, w_qkv, w_out):
    rows, width = states.shape
    inner = w_out.shape[0]
    size = inner // HEADS
    hbm = pl.BlockSpec(memory_space=pltpu.HBM)
    dma = pltpu.SemaphoreType.DMA
    return pl.pallas_call(
        kernel,
        name="episode_attention",
        out_shape=jax.ShapeDtypeStruct((rows, width), BF16),
        in_specs=[hbm] * 6,
        out_specs=pl.BlockSpec(memory_space=pltpu.VMEM),
        scratch_shapes=[
            pltpu.VMEM((rows, width), BF16),
            pltpu.VMEM((1, rows), jnp.int32),
            pltpu.VMEM(kind_table.shape, BF16),
            pltpu.VMEM((rows, width), BF16),
            pltpu.VMEM((3, CHIPS, width, 2 * size), BF16),
            pltpu.VMEM((inner, width), BF16),
            pltpu.VMEM((CHIPS, 2, 2 * size, rows), BF16),
            pltpu.VMEM((CHIPS, 2, size, rows), BF16),
            pltpu.VMEM((CHIPS, 2, size, rows), BF16),
            pltpu.VMEM((HEADS, 2 * size, rows), BF16),
            pltpu.VMEM((HEADS, size, rows), BF16),
            pltpu.VMEM((HEADS, 1, rows), jnp.int32),
            pltpu.VMEM((HEADS, size, rows), BF16),
            pltpu.VMEM((HEADS * rows, 2 * size), BF16),
            pltpu.VMEM((HEADS * rows, 2 * rows), F32),
            pltpu.VMEM((size, HEADS * rows), BF16),
            pltpu.VMEM((rows, inner), BF16),
            pltpu.VMEM((rows, width), F32),
            dma((5,)), dma((2, CHIPS)), pltpu.SemaphoreType.REGULAR((2,)),
            dma((2,)), dma((CHIPS,)),
            dma((2,)), dma((CHIPS,)),
            dma(()), dma(()),
            dma((2,)), dma((CHIPS,)),
        ],
        compiler_params=pltpu.CompilerParams(
            collective_id=0, has_side_effects=True, vmem_limit_bytes=48000000
        ),
    )(*[pltpu.with_memory_space_constraint(v, pltpu.HBM) for v in (states, token_kind.reshape(1, rows), episode.reshape(1, rows), kind_table, w_qkv, w_out)])


def solution(mesh):
    placed = (P(("dp", "seq"), None), P(("dp", "seq")), P(("dp", "seq")), P(), P(), P())
    return jax.shard_map(
        local, mesh=mesh, in_specs=placed, out_specs=P(("dp", "seq"), None), check_vma=False
    )
```

```python
import jax
import jax.numpy as jnp
from jax import lax
from jax.experimental import pallas as pl
from jax.experimental.pallas import tpu as pltpu
from jax.sharding import PartitionSpec as P

HEADS = 16
CHIPS = 8
MESH = pl.DeviceIdType.MESH
BF16 = jnp.bfloat16
F32 = jnp.float32
FAR = -1e30
AHEAD = 4


NEAR = 4
OWN = CHIPS - 1


def packed(turns):
    return sum(turn << (3 * at) for at, turn in enumerate(turns))


KV_TURNS = packed((2, 6, 1, 7, 4, 3, 5, 0))
Q_TURNS = packed((4, 3, 5, 2, 6, 1, 7, 0))


def kernel(
    states_hbm, kind_hbm, episode_hbm, table_hbm, w_qkv_hbm, w_out_hbm, out_ref,
    states_ref, kind_ref, table_ref, x_ref, w_ref, wo_ref, kv_stage, q_stage, o_stage, kv_buf, q_buf, ep_buf, o_buf,
    k_aug, s_ref, v_ref, h_ref, acc_ref,
    in_sem, w_sem, beyond, kv_send, kv_recv, q_send, q_recv, ep_send, ep_recv, o_send, o_recv,
):
    rows, width = states_ref.shape
    inner = wo_ref.shape[0]
    size = inner // HEADS
    pair = 2 * size
    block = 2 * rows
    me = lax.axis_index("seq")
    z, c = me // 2, me % 2

    barrier = pltpu.get_barrier_semaphore()

    def greet(k, _):
        pl.semaphore_signal(barrier, inc=1, device_id={"seq": (2 * z + k) % HEADS}, device_id_type=MESH)
        return 0

    partner = z * 2 + 1 - c
    lax.fori_loop(2, 6, greet, 0)
    lax.fori_loop(HEADS - 4, HEADS, greet, 0)
    pl.semaphore_signal(barrier, inc=1, device_id={"seq": partner}, device_id_type=MESH)

    def tell(side, chips):
        pl.semaphore_signal(
            beyond.at[side], inc=1, device_id={"seq": (z + chips) % CHIPS * 2 + c}, device_id_type=MESH
        )

    loads = [
        pltpu.make_async_copy(states_hbm, states_ref, in_sem.at[0]),
        pltpu.make_async_copy(kind_hbm, kind_ref, in_sem.at[1]),
        pltpu.make_async_copy(table_hbm, table_ref, in_sem.at[2]),
        pltpu.make_async_copy(episode_hbm, ep_buf.at[me], in_sem.at[3]),
    ]

    def w_out_copy(slot):
        g = to_chip(Q_TURNS, (slot + OWN) % CHIPS)
        return pltpu.make_async_copy(
            w_out_hbm.at[pl.ds(pl.multiple_of(g * pair, pair), pair)],
            wo_ref.at[pl.ds(pl.multiple_of(slot * pair, pair), pair)], in_sem.at[4],
        )

    for load in loads:
        load.start()

    def to_chip(turns, k):
        return (z + ((turns >> (3 * k)) & 7)) % CHIPS

    def from_chip(turns, k):
        return (z + CHIPS - ((turns >> (3 * k)) & 7)) % CHIPS

    def weights(k, part):
        g = to_chip(KV_TURNS if part else Q_TURNS, k)
        at = pl.multiple_of(part * inner + g * pair, pair)
        return pltpu.make_async_copy(
            w_qkv_hbm.at[:, pl.ds(at, pair)], w_ref.at[part, k], w_sem.at[0 if part == 0 else 1, k]
        )

    def landed(ref, sem):
        pltpu.make_async_copy(ref, ref, sem).wait()

    def fetch_kv(k, _):
        weights(k, 1).start()
        weights(k, 2).start()
        return 0

    lax.fori_loop(0, AHEAD, fetch_kv, 0)

    for load in loads:
        load.wait()
    kinds = jnp.broadcast_to(kind_ref[...].astype(F32), (rows, rows)).T
    for at in range(0, width, rows):
        table = table_ref[:, at : at + rows].astype(F32)
        added = jnp.broadcast_to(table[3:4], (rows, rows))
        for kind in range(3):
            added = jnp.where(kinds == float(kind), table[kind : kind + 1], added)
        x_ref[:, at : at + rows] = (states_ref[:, at : at + rows].astype(F32) + added).astype(BF16)

    def episode_copy(k, core):
        return pltpu.make_async_remote_copy(
            src_ref=ep_buf.at[me], dst_ref=ep_buf.at[me], send_sem=ep_send, recv_sem=ep_recv,
            device_id={"seq": to_chip(KV_TURNS, k) * 2 + core}, device_id_type=MESH,
        )

    def kv_copy(k, core, lane=0):
        return pltpu.make_async_remote_copy(
            src_ref=kv_stage.at[k, core], dst_ref=kv_buf.at[me], send_sem=kv_send.at[lane], recv_sem=kv_recv.at[z],
            device_id={"seq": to_chip(KV_TURNS, k) * 2 + core}, device_id_type=MESH,
        )

    def q_copy(k, core, lane=0):
        return pltpu.make_async_remote_copy(
            src_ref=q_stage.at[k, core], dst_ref=q_buf.at[me], send_sem=q_send.at[lane], recv_sem=q_recv.at[z],
            device_id={"seq": to_chip(Q_TURNS, k) * 2 + core}, device_id_type=MESH,
        )

    def o_copy(b, core, lane=0):
        return pltpu.make_async_remote_copy(
            src_ref=o_stage.at[b, core], dst_ref=o_buf.at[me], send_sem=o_send.at[lane], recv_sem=o_recv.at[z],
            device_id={"seq": 2 * b + core}, device_id_type=MESH,
        )

    def project(k, part):
        return jnp.dot(x_ref[...], w_ref[part, k], preferred_element_type=F32).astype(BF16).T

    def make_kv(k):
        landed(w_ref.at[pl.ds(1, 2), k], w_sem.at[1, k])
        keys = project(k, 1)
        values = project(k, 2)
        for core in range(2):
            kv_stage[k, core, :size] = keys[core * size : (core + 1) * size]
            kv_stage[k, core, size:] = values[core * size : (core + 1) * size]

    def make_q(k):
        landed(w_ref.at[0, k], w_sem.at[0, k])
        queries = project(k, 0)
        for core in range(2):
            q_stage[k, core] = queries[core * size : (core + 1) * size]

    def fetch_later(k):
        @pl.when(k < CHIPS)
        def _():
            weights(k, 1).start()
            weights(k, 2).start()

        @pl.when((k >= CHIPS) & (k < 2 * CHIPS))
        def _():
            weights(k - CHIPS, 0).start()

    def send_kv(k, _):
        @pl.when(k == NEAR)
        def _():
            pl.semaphore_wait(beyond.at[0], 1)
            pl.semaphore_wait(beyond.at[1], 1)

        episode_copy(k, 0).start()
        episode_copy(k, 1).start()
        kv_copy(k, 0).start()
        kv_copy(k, 1).start()
        return 0

    def send_q(k, _):
        q_copy(k, 0).start()
        q_copy(k, 1).start()
        return 0

    def stage_kv(k, _):
        fetch_later(k + AHEAD)
        make_kv(k)
        return 0

    def stage_q(k, _):
        fetch_later(k + CHIPS + AHEAD)
        make_q(k)
        return 0

    def do_kv(k, _):
        stage_kv(k, 0)
        return send_kv(k, 0)

    def do_q(k, _):
        stage_q(k, 0)
        return send_q(k, 0)

    late = (z == 0) & (c == 0) & (lax.axis_index("dp") == 0)
    kv_early = jnp.where(z < 3, 7, jnp.where(z == 3, 5, jnp.where(z < 6, 2, 1)))
    kv_early = jnp.where(late, 2, kv_early)
    q_early = jnp.where((z < 2) & jnp.logical_not(late), 7, 0)
    own_early = (z < 3) & jnp.logical_not(late)
    lax.fori_loop(0, kv_early, stage_kv, 0)

    @pl.when(own_early)
    def _():
        stage_kv(7, 0)

    lax.fori_loop(0, q_early, stage_q, 0)

    pl.semaphore_wait(barrier, 9)
    tell(0, 2)
    tell(1, 6)
    lax.fori_loop(0, kv_early, send_kv, 0)
    lax.fori_loop(kv_early, 7, do_kv, 0)

    @pl.when(jnp.logical_not(own_early))
    def _():
        stage_kv(7, 0)

    episode_copy(7, 1 - c).start()
    kv_copy(7, 1 - c, 1).start()
    kv_buf[me] = kv_stage[7, c]
    lax.fori_loop(0, q_early, send_q, 0)
    lax.fori_loop(q_early, 7, do_q, 0)

    stage_q(7, 0)
    q_copy(7, 1 - c, 1).start()
    q_buf[me] = q_stage[7, c]

    def fetch_w_out(slot, _):
        w_out_copy(slot).start()
        return 0

    lax.fori_loop(0, CHIPS, fetch_w_out, 0)

    lines = lax.broadcasted_iota(jnp.int32, (size, rows), 0)

    def take_kv(j):
        other = jnp.where((lines < 4) & (lines != ep_buf[j]), 1.0, 0.0).astype(BF16)
        at = pl.multiple_of(j * rows, rows)
        k_aug[pl.ds(at, rows)] = jnp.concatenate([kv_buf[j, :size], other], axis=0).T
        v_ref[:size, pl.ds(at, rows)] = kv_buf[j, size:]

    def take_chip(k, _):
        g = from_chip(KV_TURNS, k)
        landed(kv_buf.at[pl.ds(2 * g, 2)], kv_recv.at[g])
        take_kv(2 * g)
        take_kv(2 * g + 1)
        return 0

    v_ref[size:] = jnp.ones((16, HEADS * rows), BF16)
    landed(ep_buf.at[pl.ds(0, HEADS - 1)], ep_recv)
    take_kv(me)
    landed(kv_buf.at[partner], kv_recv.at[z])
    take_kv(partner)
    lax.fori_loop(0, 7, take_chip, 0)

    later = lax.broadcasted_iota(jnp.int32, (block, block), 0) > lax.broadcasted_iota(jnp.int32, (block, block), 1)

    def attend(b):
        queries = []
        for j in (2 * b, 2 * b + 1):
            same = jnp.where(lines == ep_buf[j], FAR, 0.0).astype(BF16)
            queries.append(jnp.concatenate([q_buf[j] * 0.125, same], axis=0))
        queries = jnp.concatenate(queries, axis=1)
        top = None
        for a in (b, *range(b)):
            scores = jnp.dot(k_aug[a * block : (a + 1) * block], queries, preferred_element_type=F32)
            if a == b:
                scores = jnp.where(later, FAR, scores)
            s_ref[a * block : (a + 1) * block] = scores
            here = jnp.max(scores.reshape(block // 8, 8, block), axis=0)
            top = here if top is None else jnp.maximum(top, here)
        top = jnp.max(top, axis=0, keepdims=True)
        summed = None
        for a in range(b + 1):
            weight = jnp.exp(s_ref[a * block : (a + 1) * block] - top)
            mixed = jnp.dot(v_ref[:, a * block : (a + 1) * block], weight.astype(BF16), preferred_element_type=F32)
            summed = mixed if summed is None else summed + mixed
        result = (summed[:size] / summed[size : size + 1]).astype(BF16)
        for core in range(2):
            o_stage[b, core] = result[:, core * rows : (core + 1) * rows]

    def attend_any(b):
        lax.switch(b, [lambda b=b: attend(b) for b in range(CHIPS)])

    landed(q_buf.at[partner], q_recv.at[z])
    attend_any(z)
    o_copy(z, 1 - c, 1).start()
    o_buf[me] = o_stage[z, c]

    def answer(k, _):
        b = from_chip(Q_TURNS, k)
        landed(q_buf.at[pl.ds(2 * b, 2)], q_recv.at[b])
        attend_any(b)
        o_copy(b, 0).start()
        o_copy(b, 1).start()
        return 0

    lax.fori_loop(0, 7, answer, 0)

    def take_o(g, slot):
        h_ref[:, pl.ds(pl.multiple_of(slot * pair, pair), pair)] = jnp.concatenate(
            [o_buf[2 * g], o_buf[2 * g + 1]], axis=0
        ).T

    def take_chip_o(k, _):
        g = to_chip(Q_TURNS, k)
        landed(o_buf.at[pl.ds(2 * g, 2)], o_recv.at[g])
        take_o(g, k + 1)
        return 0

    landed(wo_ref, in_sem.at[4])
    landed(o_buf.at[partner], o_recv.at[z])
    take_o(z, 0)
    lax.fori_loop(0, 5, take_chip_o, 0)
    most = 6 * pair
    acc_ref[...] = jnp.dot(h_ref[:, :most], wo_ref[:most], preferred_element_type=F32)
    lax.fori_loop(5, 7, take_chip_o, 0)
    rest = jnp.dot(h_ref[:, most:], wo_ref[most:], preferred_element_type=F32)
    out_ref[...] = (acc_ref[...] + rest).astype(BF16)

    landed(ep_buf.at[pl.ds(0, HEADS - 1)], ep_send)
    landed(kv_stage.at[pl.ds(0, 7)], kv_send.at[0])
    landed(q_stage.at[pl.ds(0, 7)], q_send.at[0])
    landed(o_stage.at[pl.ds(0, 7)], o_send.at[0])
    landed(kv_stage.at[7, 0], kv_send.at[1])
    landed(q_stage.at[7, 0], q_send.at[1])
    landed(o_stage.at[7, 0], o_send.at[1])


def local(states, token_kind, episode, kind_table, w_qkv, w_out):
    rows, width = states.shape
    inner = w_out.shape[0]
    size = inner // HEADS
    hbm = pl.BlockSpec(memory_space=pltpu.HBM)
    dma = pltpu.SemaphoreType.DMA
    return pl.pallas_call(
        kernel,
        name="episode_attention",
        out_shape=jax.ShapeDtypeStruct((rows, width), BF16),
        in_specs=[hbm] * 6,
        out_specs=pl.BlockSpec(memory_space=pltpu.VMEM),
        scratch_shapes=[
            pltpu.VMEM((rows, width), BF16),
            pltpu.VMEM((1, rows), jnp.int32),
            pltpu.VMEM(kind_table.shape, BF16),
            pltpu.VMEM((rows, width), BF16),
            pltpu.VMEM((3, CHIPS, width, 2 * size), BF16),
            pltpu.VMEM((inner, width), BF16),
            pltpu.VMEM((CHIPS, 2, 2 * size, rows), BF16),
            pltpu.VMEM((CHIPS, 2, size, rows), BF16),
            pltpu.VMEM((CHIPS, 2, size, rows), BF16),
            pltpu.VMEM((HEADS, 2 * size, rows), BF16),
            pltpu.VMEM((HEADS, size, rows), BF16),
            pltpu.VMEM((HEADS, 1, rows), jnp.int32),
            pltpu.VMEM((HEADS, size, rows), BF16),
            pltpu.VMEM((HEADS * rows, 2 * size), BF16),
            pltpu.VMEM((HEADS * rows, 2 * rows), F32),
            pltpu.VMEM((size + 16, HEADS * rows), BF16),
            pltpu.VMEM((rows, inner), BF16),
            pltpu.VMEM((rows, width), F32),
            dma((5,)), dma((2, CHIPS)), pltpu.SemaphoreType.REGULAR((2,)),
            dma((2,)), dma((CHIPS,)),
            dma((2,)), dma((CHIPS,)),
            dma(()), dma(()),
            dma((2,)), dma((CHIPS,)),
        ],
        compiler_params=pltpu.CompilerParams(
            collective_id=0, has_side_effects=True, vmem_limit_bytes=48000000
        ),
    )(*[pltpu.with_memory_space_constraint(v, pltpu.HBM) for v in (states, token_kind.reshape(1, rows), episode.reshape(1, rows), kind_table, w_qkv, w_out)])


def solution(mesh):
    placed = (P(("dp", "seq"), None), P(("dp", "seq")), P(("dp", "seq")), P(), P(), P())
    return jax.shard_map(
        local, mesh=mesh, in_specs=placed, out_specs=P(("dp", "seq"), None), check_vma=False
    )
```
